128 devices in a mesh: dp: 16 (over x, z), tensor: 8 (over y, core).
Axes of the slice: x: 4, y: 4, z: 4, core: 2. Of those that a mesh axis runs over, the one named last changes fastest.
Arguments:
- tokens: bfloat16 [1024, 4096], P('dp', 'tensor')
- norm_gain: float32 [4096], P('tensor'), may hold values from 0.5 to 1.5
- eraser_mean: float32 [4096], P('tensor'), may hold values from -6 to 6
- eraser_in: float32 [4096, 128], P('tensor'), may hold values from -0.09375 to 0.09375
- eraser_out: float32 [4096, 128], P('tensor'), may hold values from -0.5 to 0.5
- router: float32 [4096, 8], P('tensor'), may hold values from -0.09375 to 0.09375
- expert_ids: int32 [1024, 2], P('dp'), may hold values from 0 to 7, as said below
- slots: int32 [1024, 2], P('dp'), may hold values from 0 to 63, as said below
- w_gate: bfloat16 [16, 4096, 7168], P('dp', None, 'tensor'), may hold values from -0.09375 to 0.09375
- w_up: bfloat16 [16, 4096, 7168], P('dp', None, 'tensor'), may hold values from -0.09375 to 0.09375
- w_down: bfloat16 [16, 7168, 4096], P('dp', 'tensor'), may hold values from -0.0625 to 0.0625
Outputs:
- moe_out: bfloat16 [1024, 4096], P('dp', 'tensor')
The draws below stay inside these ranges and needn't reach their ends.
Inputs may be any that keep to these rules, and one draw needn't show every extreme that they name: `expert_ids`: the two experts of a token differ. Within each aligned block of 64 tokens, the choices naming one expert have the slots 0, 1, 2, ... with no repeats; choices with a slot of 24 or more are dropped.
All inputs are finite; a program needn't handle non-finite values.
Results may differ from the reference program's by a relative error of at most 0.0065.
Values may be sent and summed in bfloat16 or wider, within the bound.
No kernel may reach another device: no remote copies, remote signals or barrier semaphores. Data moves between devices by JAX's collectives and lax.ppermute only.
A program may use at most 128 MiB of HBM per device.

```python
import jax
import jax.numpy as jnp
from jax import lax

D = 4096
FF = 14336
E = 8
K = 128
TOK_DEV = 64
CAP = 24
FF_PARTS = 2
TOKENS = 1024


def route_table(key):
    folded = jax.random.fold_in(key, 11)
    key_hot, key_bias, key_jitter, key_order = jax.random.split(folded, 4)
    expert_range = jnp.arange(E, dtype=jnp.int32)
    hot_expert = jax.random.randint(key_hot, (), 0, E, dtype=jnp.int32)
    expert_bias = jax.random.randint(key_bias, (E,), 0, 24, dtype=jnp.int32) + 200 * (expert_range == hot_expert).astype(jnp.int32)
    jitter = jax.random.randint(key_jitter, (TOKENS, E), 0, 64, dtype=jnp.int32)
    scores = (jitter + expert_bias[None, :]) * E + expert_range[None, :]
    unused, chosen = lax.top_k(scores, 2)
    chosen = chosen.astype(jnp.int32)
    priority = jax.random.randint(key_order, (TOKENS,), 0, 4096, dtype=jnp.int32) * TOKENS + jnp.arange(TOKENS, dtype=jnp.int32)
    blocks = TOKENS // TOK_DEV
    onehot = jnp.sum((chosen[:, :, None] == expert_range[None, None, :]).astype(jnp.int32), axis=1).reshape(blocks, TOK_DEV, E)
    ordered = priority.reshape(blocks, TOK_DEV)
    earlier = (ordered[:, None, :] < ordered[:, :, None]).astype(jnp.int32)
    ranks = jnp.sum(earlier[:, :, :, None] * onehot[:, None, :, :], axis=2).reshape(TOKENS, E)
    slot_table = jnp.take_along_axis(ranks, chosen, axis=1).astype(jnp.int32)
    return (chosen, slot_table)


def draw_expert_ids(key, part):
    return route_table(key)[0]


def draw_slots(key, part):
    return route_table(key)[1]


def draw_tokens(key, part):
    key_rows, key_cols, key_base = jax.random.split(jax.random.fold_in(key, 5), 3)
    col_scale = 3.0 ** (jnp.arange(D, dtype=jnp.float32) / D) * jnp.exp(jax.random.uniform(key_cols, (1, D), jnp.float32, -0.5, 0.5))
    row_scale = jnp.exp(jax.random.uniform(key_rows, (TOKENS, 1), jnp.float32) * jnp.log(10.0))
    base = jnp.clip(jax.random.normal(key_base, (TOKENS, D), jnp.float32), -5.0, 5.0)
    return (base * row_scale * col_scale).astype(jnp.bfloat16)


def spiked(drawn, stream_key, source, target, shards_of, factor):
    owner, partner = [(jnp.arange(drawn.shape[dim]) // (drawn.shape[dim] // shards_of)).reshape([-1 if axis == dim else 1 for axis in range(drawn.ndim)]) for dim in (source, target)]
    chosen = jax.random.permutation(stream_key, shards_of)[partner]
    strong = (owner == chosen) | (owner == (partner + shards_of // 2) % shards_of)
    return jnp.where(strong, factor * drawn, drawn)


def steps_of(rng, extent, shards, smallest, top_value):
    def one(dim, shards_of):
        heights = jax.random.uniform(jax.random.fold_in(jax.random.fold_in(rng, 6), dim), (shards_of,), jnp.float32, smallest / len(shards), top_value / len(shards))
        return jnp.repeat(jnp.exp(heights), extent[dim] // shards_of).reshape((-1,) + (1,) * (len(extent) - dim - 1))

    gain = one(*shards[0])
    for cut in shards[1:]:
        gain = gain * one(*cut)
    return gain


def noise(key, shape, deviation, reach, cuts=(), held_as=jnp.bfloat16):
    level = steps_of(key, shape, cuts, -0.22, 0.18) if cuts else 1.0
    entries = jax.random.normal(key, shape, jnp.float32) * deviation * level
    return jnp.minimum(jnp.maximum(entries, -reach), reach).astype(held_as)


def heavy_noise(own_key, dims, scale, limit, cuts, heavy, kind=jnp.bfloat16):
    entries = scale * jax.random.normal(own_key, dims, jnp.float32)
    if cuts:
        entries = entries * steps_of(own_key, dims, cuts, -0.22, 0.18)
    return jnp.clip(spiked(entries, jax.random.fold_in(own_key, 3), *heavy), -limit, limit).astype(kind)


def setup_inputs(seed: int = 0) -> dict:
    streams_of = jax.random.split(jax.random.key(seed), 12)
    return {
        "tokens": draw_tokens(jax.random.fold_in(streams_of[11], 71), 0),
        "norm_gain": jnp.clip(1.0 + 0.1 * jax.random.normal(streams_of[1], (D,), jnp.float32), 0.5, 1.5),
        "eraser_mean": noise(streams_of[2], (D,), 1.0, 6.0, ((0, 8),), jnp.float32),
        "eraser_in": noise(streams_of[3], (D, K), D ** -0.5, 0.09375, ((0, 8),), jnp.float32),
        "eraser_out": noise(streams_of[4], (D, K), K ** -0.5, 0.5, ((0, 8),), jnp.float32),
        "router": noise(streams_of[5], (D, E), D ** -0.5, 0.09375, ((0, 8),), jnp.float32),
        "expert_ids": draw_expert_ids(jax.random.fold_in(streams_of[11], 71), 0),
        "slots": draw_slots(jax.random.fold_in(streams_of[11], 71), 0),
        "w_gate": noise(streams_of[8], (E * FF_PARTS, D, FF // FF_PARTS), D ** -0.5, 0.09375, ((0, 16), (2, 8))),
        "w_up": noise(streams_of[9], (E * FF_PARTS, D, FF // FF_PARTS), D ** -0.5, 0.09375, ((0, 16), (2, 8))),
        "w_down": heavy_noise(streams_of[10], (E * FF_PARTS, FF // FF_PARTS, D), FF ** -0.5, 0.0625, ((0, 16), (1, 8)), (1, 2, 8, 2.0)),
    }


def reference(tokens, norm_gain, eraser_mean, eraser_in, eraser_out, router, expert_ids, slots, w_gate, w_up, w_down):
    highest = lax.Precision.HIGHEST
    values = tokens.astype(jnp.float32)
    inv_rms = lax.rsqrt(lax.optimization_barrier(jnp.mean(values * values, axis=1, keepdims=True)) + 1e-05)
    normed = values * norm_gain[None, :] * inv_rms
    projected = jnp.dot(normed - eraser_mean[None, :], eraser_in, precision=highest, preferred_element_type=jnp.float32)
    cleaned = normed - jnp.dot(projected, eraser_out.T, precision=highest, preferred_element_type=jnp.float32)
    erased = cleaned.astype(jnp.bfloat16)
    logits = jnp.dot(cleaned, router, precision=highest, preferred_element_type=jnp.float32)
    chosen = (expert_ids[:, :, None] == jnp.arange(E, dtype=jnp.int32)[None, None, :]).astype(jnp.float32)
    picked = lax.optimization_barrier(jnp.sum(chosen * logits[:, None, :], axis=2))
    first_gate = jax.nn.sigmoid(picked[:, 0] - picked[:, 1])
    gate_pair = jnp.stack([first_gate, 1.0 - first_gate], axis=1)
    kept_mask = slots < CAP
    blocks = TOKENS // TOK_DEV
    block_index = (jnp.arange(TOKENS, dtype=jnp.int32) // TOK_DEV).astype(jnp.int32)
    target = block_index[:, None] * CAP + slots
    columns = jnp.arange(blocks * CAP, dtype=jnp.int32)
    erased_wide = erased.astype(jnp.float32)
    combined = jnp.zeros((TOKENS, D), jnp.float32)
    for expert in range(E):
        match = ((target[:, :, None] == columns[None, None, :]) & ((expert_ids == expert) & kept_mask)[:, :, None]).astype(jnp.float32)
        placing = lax.optimization_barrier(jnp.sum(match, axis=1))
        weights = lax.optimization_barrier(jnp.sum(match * gate_pair[:, :, None], axis=1))
        buffer = jnp.dot(placing.T, erased_wide, precision=highest, preferred_element_type=jnp.float32)
        outputs = jnp.zeros((blocks * CAP, D), jnp.float32)
        for piece in range(FF_PARTS):
            index = expert * FF_PARTS + piece
            gate_act = jnp.dot(buffer, w_gate[index].astype(jnp.float32), precision=highest, preferred_element_type=jnp.float32)
            up_act = jnp.dot(buffer, w_up[index].astype(jnp.float32), precision=highest, preferred_element_type=jnp.float32)
            hidden = (jax.nn.silu(gate_act) * up_act).astype(jnp.bfloat16)
            outputs = outputs + jnp.dot(hidden.astype(jnp.float32), w_down[index].astype(jnp.float32), precision=highest, preferred_element_type=jnp.float32)
        combined = combined + jnp.dot(weights, outputs, precision=highest, preferred_element_type=jnp.float32)
    return combined.astype(jnp.bfloat16)
```

```python
import jax
import jax.numpy as jnp
from jax import lax
from jax.sharding import PartitionSpec as P

E = 8
HIGHEST = lax.Precision.HIGHEST


def dot32(a, b):
    return jnp.dot(a, b, precision=HIGHEST, preferred_element_type=jnp.float32)


def on_device(tokens, norm_gain, eraser_mean, eraser_in, eraser_out, router, expert_ids, slots, w_gate, w_up, w_down):
    bf = jnp.bfloat16
    f32 = jnp.float32
    n_t = lax.axis_size("tensor")
    n_y = n_t // 2
    part_count = lax.axis_size("dp") // E
    rows, width = tokens.shape
    capacity = 3 * rows // 8
    full = width * n_t
    total = lax.axis_size("dp") * capacity
    rank = eraser_in.shape[1]
    t = lax.axis_index("tensor")
    y, c = t // 2, t % 2

    def along_y(v, k):
        return lax.ppermute(v, "tensor", [(s, ((s // 2 + k) % n_y) * 2 + s % 2) for s in range(n_t)])

    def to_twin(v):
        return lax.ppermute(v, "tensor", [(s, s ^ 1) for s in range(n_t)])

    values = tokens.astype(f32)
    gained = values * norm_gain[None, :]
    squares = jnp.sum(values * values, axis=1)
    left = jnp.concatenate([gained, jnp.broadcast_to(eraser_mean[None, :], (8, width)), router.T], axis=0)
    part = dot32(left, eraser_in)
    gained_in, mean_in = part[:rows], part[rows : rows + 1]
    gained_router = dot32(router.T, gained.T)
    out_router_t = dot32(router.T, eraser_out)
    extra = jnp.concatenate([gained_router, jnp.broadcast_to(squares[None, :], (8, rows))], axis=0)
    extra = jnp.concatenate([extra, jnp.zeros((16, rank - rows), f32)], axis=1)
    packed = jnp.concatenate([part[: rows + 8], out_router_t, extra], axis=0)
    copies = jnp.broadcast_to(packed[None], (n_t, *packed.shape))
    packed = jnp.sum(lax.all_to_all(copies, "tensor", split_axis=0, concat_axis=0, tiled=True), axis=0)
    gained_in, mean_in = packed[:rows], packed[rows : rows + 1]
    out_router_t = packed[rows + 8 : rows + 16]
    gained_router_t = packed[rows + 16 : rows + 24, :rows]
    squares = packed[rows + 24, :rows]
    inv_rms = lax.rsqrt(squares / full + 1e-05)
    projected = inv_rms[:, None] * gained_in - mean_in
    cleaned = inv_rms[:, None] * gained - lax.dot_general(
        projected, eraser_out, (((1,), (1,)), ((), ())), precision=HIGHEST, preferred_element_type=f32
    )
    erased = cleaned.astype(bf)
    logits = inv_rms[:, None] * gained_router_t.T - lax.dot_general(
        projected, out_router_t, (((1,), (1,)), ((), ())), precision=HIGHEST, preferred_element_type=f32
    )
    chosen = (expert_ids[:, :, None] == jnp.arange(E, dtype=jnp.int32)[None, None, :]).astype(f32)
    picked = jnp.sum(chosen * logits[:, None, :], axis=2)
    first_gate = jax.nn.sigmoid(picked[:, 0] - picked[:, 1])
    gate_pair = jnp.stack([first_gate, 1.0 - first_gate], axis=1)
    kept = slots < capacity
    place = jnp.arange(total, dtype=jnp.int32)
    place = (place // capacity // part_count) * capacity + place % capacity
    target = jnp.where(kept, expert_ids * capacity + slots, -1)
    match = (target[:, :, None] == place[None, None, :]).astype(f32)
    placing = jnp.sum(match, axis=1).astype(bf)
    weights = jnp.sum(match * gate_pair[:, :, None], axis=1)

    sent = lax.dot_general(placing, erased, (((0,), (0,)), ((), ())), preferred_element_type=f32).astype(bf)
    own = lax.all_to_all(sent, "dp", split_axis=0, concat_axis=0, tiled=True)

    half = total // 2
    up = along_y(own, 1)
    down = along_y(own, -1)
    own2 = to_twin(own)
    far_a = along_y(up[:half], 1)
    far_b = along_y(down[half:], -1)
    up2 = to_twin(up)
    down2 = to_twin(down)
    far = jnp.concatenate([far_a, far_b], axis=0)
    far2 = to_twin(far)
    buf = jnp.zeros((total, full), bf)
    for k, pair in ((0, (own, own2)), (-1, (up, up2)), (1, (down, down2)), (2, (far, far2))):
        base = ((y + k) % n_y) * 2
        buf = lax.dynamic_update_slice(buf, pair[0], (0, (base + c) * width))
        buf = lax.dynamic_update_slice(buf, pair[1], (0, (base + 1 - c) * width))
    gate_act = jnp.dot(buf, w_gate[0], preferred_element_type=f32)
    up_act = jnp.dot(buf, w_up[0], preferred_element_type=f32)
    hidden = (jax.nn.silu(gate_act) * up_act).astype(bf)
    outputs = jnp.dot(hidden, w_down[0], preferred_element_type=f32)

    outputs = outputs.reshape(total, n_y, 2, width)
    mine = lax.dynamic_index_in_dim(outputs, c, 2, keepdims=False)
    other = lax.dynamic_index_in_dim(outputs, 1 - c, 2, keepdims=False).astype(bf)
    mine = mine + to_twin(other).astype(f32)

    def piece(k):
        return lax.dynamic_index_in_dim(mine, (y + k) % n_y, 1, keepdims=False)

    far = piece(2).astype(bf)
    got_far_a = along_y(far[:half], 1)
    got_far_b = along_y(far[half:], -1)
    to_up = piece(1)
    to_down = piece(-1)
    to_up = jnp.concatenate([to_up[:half] + got_far_a.astype(f32), to_up[half:]], axis=0).astype(bf)
    to_down = jnp.concatenate([to_down[:half], to_down[half:] + got_far_b.astype(f32)], axis=0).astype(bf)
    reduced = piece(0) + along_y(to_up, 1).astype(f32) + along_y(to_down, -1).astype(f32)
    returned = lax.all_to_all(reduced.astype(bf), "dp", split_axis=0, concat_axis=0, tiled=True)
    mixed = jnp.dot(weights, returned.astype(f32), precision=HIGHEST, preferred_element_type=f32)
    return mixed.astype(bf)


def solution(mesh):
    in_specs = (
        P("dp", "tensor"),
        P("tensor"),
        P("tensor"),
        P("tensor", None),
        P("tensor", None),
        P("tensor", None),
        P("dp", None),
        P("dp", None),
        P("dp", None, "tensor"),
        P("dp", None, "tensor"),
        P("dp", "tensor", None),
    )
    return jax.shard_map(on_device, mesh=mesh, in_specs=in_specs, out_specs=P("dp", "tensor"), check_vma=False)
```

```python
import jax
import jax.numpy as jnp
from jax import lax
from jax.experimental import pallas as pl
from jax.sharding import PartitionSpec as P

E = 8
HIGHEST = lax.Precision.HIGHEST


def dot32(a, b):
    return jnp.dot(a, b, precision=HIGHEST, preferred_element_type=jnp.float32)


def dot32_nt(a, b):
    return lax.dot_general(a, b, (((1,), (1,)), ((), ())), precision=HIGHEST, preferred_element_type=jnp.float32)


def sums_kernel(tokens, gain, mean, eraser_in, eraser_out, router_t, out):
    rows = tokens.shape[0]
    values = tokens[...].astype(jnp.float32)
    gained = values * gain[...]
    out[:rows] = dot32(gained, eraser_in[...])
    out[rows : rows + 8] = dot32(jnp.broadcast_to(mean[...], (8, mean.shape[1])), eraser_in[...])
    out[rows + 8 : rows + 16] = dot32(router_t[...], eraser_out[...])
    out[rows + 16 : rows + 24, :rows] = dot32_nt(router_t[...], gained)
    out[rows + 16 : rows + 24, rows : 2 * rows] = dot32_nt(jnp.ones((8, values.shape[1]), jnp.float32), values * values)


def on_device(tokens, norm_gain, eraser_mean, eraser_in, eraser_out, router, expert_ids, slots, w_gate, w_up, w_down):
    bf = jnp.bfloat16
    f32 = jnp.float32
    n_t = lax.axis_size("tensor")
    n_y = n_t // 2
    part_count = lax.axis_size("dp") // E
    rows, width = tokens.shape
    capacity = 3 * rows // 8
    full = width * n_t
    total = lax.axis_size("dp") * capacity
    rank = eraser_in.shape[1]
    t = lax.axis_index("tensor")
    y, c = t // 2, t % 2

    def along_y(v, k):
        return lax.ppermute(v, "tensor", [(s, ((s // 2 + k) % n_y) * 2 + s % 2) for s in range(n_t)])

    def to_twin(v):
        return lax.ppermute(v, "tensor", [(s, s ^ 1) for s in range(n_t)])

    target = jnp.where(slots < capacity, expert_ids * capacity + slots, -1)
    place = jnp.arange(total, dtype=jnp.int32)
    place = (place // capacity // part_count) * capacity + place % capacity
    match = target.T[:, None, :] == place[None, :, None]
    placing = lax.optimization_barrier(jnp.any(match, axis=0).astype(bf))
    packed = pl.pallas_call(
        sums_kernel, out_shape=jax.ShapeDtypeStruct((rows + 24, rank), f32), name="sums"
    )(tokens, norm_gain[None, :], eraser_mean[None, :], eraser_in, eraser_out, router.T)
    packed = packed + to_twin(packed)
    sums = (packed + along_y(packed, 2)) + (along_y(packed, 1) + along_y(packed, -1))
    mean_in = sums[rows : rows + 1]
    out_router_t = sums[rows + 8 : rows + 16]
    inv_rms = lax.rsqrt(sums[rows + 16, rows : 2 * rows] / full + 1e-05)
    projected = inv_rms[:, None] * sums[:rows] - mean_in
    gained = tokens.astype(f32) * norm_gain[None, :]
    erased = (inv_rms[:, None] * gained - dot32_nt(projected, eraser_out)).astype(bf)
    sent = jnp.dot(placing, erased, preferred_element_type=f32).astype(bf)
    own = lax.all_to_all(sent.reshape(-1, capacity, width), "dp", split_axis=0, concat_axis=0, tiled=True)
    own = own.reshape(total, width)

    logits = inv_rms[:, None] * sums[rows + 16 : rows + 24, :rows].T - lax.dot_general(
        projected, out_router_t, (((1,), (1,)), ((), ())), precision=HIGHEST, preferred_element_type=f32
    )
    chosen = (expert_ids[:, :, None] == jnp.arange(E, dtype=jnp.int32)[None, None, :]).astype(f32)
    picked = jnp.sum(chosen * logits[:, None, :], axis=2)
    first_gate = jax.nn.sigmoid(picked[:, 0] - picked[:, 1])
    gate_pair = jnp.stack([first_gate, 1.0 - first_gate], axis=1)
    weights = jnp.sum((target[:, :, None] == place[None, None, :]).astype(f32) * gate_pair[:, :, None], axis=1)

    half = total // 2
    wg, wu, wd = w_gate[0], w_up[0], w_down[0]

    def rows_of(w, k, core):
        return lax.dynamic_slice_in_dim(w, (((y + k) % n_y) * 2 + core) * width, width, 0)

    def cols_of(w, k, core):
        return lax.dynamic_slice_in_dim(w, (((y + k) % n_y) * 2 + core) * width, width, 1)

    def dot(p, q):
        return jnp.dot(p, q, preferred_element_type=f32)

    def add_to(acc, *pieces):
        for piece, k, core in pieces:
            g = dot(piece, rows_of(wg, k, core))
            u = dot(piece, rows_of(wu, k, core))
            acc = (g, u) if acc is None else (acc[0] + g, acc[1] + u)
        return acc

    up_a = along_y(own[:half], 1)
    down_b = along_y(own[half:], -1)
    up_b = along_y(own[half:], 1)
    down_a = along_y(own[:half], -1)
    own2 = to_twin(own)
    acc = add_to(None, (own, 0, c), (own2, 0, 1 - c))
    far_a = along_y(up_a, 1)
    far_b = along_y(down_b, -1)
    up = jnp.concatenate([up_a, up_b], axis=0)
    down = jnp.concatenate([down_a, down_b], axis=0)
    up, down, acc = lax.optimization_barrier((up, down, acc))
    up2 = to_twin(up)
    down2 = to_twin(down)
    acc = add_to(acc, (up, -1, c), (down, 1, c), (up2, -1, 1 - c), (down2, 1, 1 - c))
    far_a, far_b, acc = lax.optimization_barrier((far_a, far_b, acc))
    far = jnp.concatenate([far_a, far_b], axis=0)
    far2 = to_twin(far)
    gate_act, up_act = add_to(acc, (far, 2, c), (far2, 2, 1 - c))
    hidden = (jax.nn.silu(gate_act) * up_act).astype(bf)

    def summed(k):
        other = dot(hidden, cols_of(wd, k, 1 - c)).astype(bf)
        return dot(hidden, cols_of(wd, k, c)) + to_twin(other).astype(f32)

    far = summed(2).astype(bf)
    got_far_a = along_y(far[:half], 1)
    got_far_b = along_y(far[half:], -1)
    to_up = summed(1)
    to_down = summed(-1)
    got_b = along_y(to_up[half:].astype(bf), 1)
    got_a = along_y(to_down[:half].astype(bf), -1)
    mine = summed(0)
    last_a = along_y((to_up[:half] + got_far_a.astype(f32)).astype(bf), 1)
    last_b = along_y((to_down[half:] + got_far_b.astype(f32)).astype(bf), -1)
    reduced = mine + jnp.concatenate(
        [last_a.astype(f32) + got_a.astype(f32), got_b.astype(f32) + last_b.astype(f32)], axis=0
    )
    returned = lax.all_to_all(
        reduced.astype(bf).reshape(-1, capacity, width), "dp", split_axis=0, concat_axis=0, tiled=True
    )
    mixed = jnp.dot(weights, returned.reshape(total, width).astype(f32), precision=HIGHEST, preferred_element_type=f32)
    return mixed.astype(bf)


def solution(mesh):
    in_specs = (
        P("dp", "tensor"),
        P("tensor"),
        P("tensor"),
        P("tensor", None),
        P("tensor", None),
        P("tensor", None),
        P("dp", None),
        P("dp", None),
        P("dp", None, "tensor"),
        P("dp", None, "tensor"),
        P("dp", "tensor", None),
    )

    return jax.shard_map(on_device, mesh=mesh, in_specs=in_specs, out_specs=P("dp", "tensor"), check_vma=False)
```

```python
import jax
import jax.numpy as jnp
from jax import lax
from jax.experimental import pallas as pl
from jax.experimental.pallas import tpu as pltpu
from jax.sharding import PartitionSpec as P

E = 8
HIGHEST = lax.Precision.HIGHEST


def dot32(a, b):
    return jnp.dot(a, b, precision=HIGHEST, preferred_element_type=jnp.float32)


def dot32_nt(a, b):
    return lax.dot_general(a, b, (((1,), (1,)), ((), ())), precision=HIGHEST, preferred_element_type=jnp.float32)


def sums_kernel(tokens, gain, mean, eraser_in, eraser_out, router_t, out, gained_out, eraser_out_copy):
    rows = tokens.shape[0]
    values = tokens[...].astype(jnp.float32)
    gained = values * gain[...]
    out[:rows] = dot32(gained, eraser_in[...])
    out[rows : rows + 8] = dot32(jnp.broadcast_to(mean[...], (8, mean.shape[1])), eraser_in[...])
    out[rows + 8 : rows + 16] = dot32(router_t[...], eraser_out[...])
    gained_out[...] = gained
    eraser_out_copy[...] = eraser_out[...]
    out[rows + 16 : rows + 24, :rows] = dot32_nt(router_t[...], gained)
    out[rows + 16 : rows + 24, rows : 2 * rows] = dot32_nt(jnp.ones((8, values.shape[1]), jnp.float32), values * values)


def on_device(tokens, norm_gain, eraser_mean, eraser_in, eraser_out, router, expert_ids, slots, w_gate, w_up, w_down):
    bf = jnp.bfloat16
    f32 = jnp.float32
    n_t = lax.axis_size("tensor")
    part_count = lax.axis_size("dp") // E
    rows, width = tokens.shape
    capacity = 3 * rows // 8
    full = width * n_t
    total = lax.axis_size("dp") * capacity
    rank = eraser_in.shape[1]
    t = lax.axis_index("tensor").astype(jnp.uint32)
    first = [(t ^ jnp.uint32(v)) * jnp.uint32(width) for v in range(n_t)]
    zero = t & jnp.uint32(0)
    tokens, zero, *first = lax.optimization_barrier((tokens, zero, *first))

    def swap_y(v, k):
        return lax.ppermute(v, "tensor", [(s, s ^ (2 * k)) for s in range(n_t)])

    def to_twin(v):
        return lax.ppermute(v, "tensor", [(s, s ^ 1) for s in range(n_t)])

    target = jnp.where(slots < capacity, expert_ids * capacity + slots, -1)
    place = jnp.arange(total, dtype=jnp.int32)
    place = (place // capacity // part_count) * capacity + place % capacity
    match = target.T[:, None, :] == place[None, :, None]
    placing = lax.optimization_barrier(jnp.any(match, axis=0).astype(bf))
    packed, gained, eraser_out = pl.pallas_call(
        sums_kernel,
        out_shape=[pltpu.VMEM((rows + 24, rank), f32), pltpu.VMEM((rows, width), f32), pltpu.VMEM((width, rank), f32)],
        out_specs=[pl.BlockSpec(memory_space=pltpu.VMEM)] * 3,
        name="sums",
    )(tokens, norm_gain[None, :], eraser_mean[None, :], eraser_in, eraser_out, router.T)
    packed = packed + to_twin(packed)
    sums = (packed + swap_y(packed, 2)) + (swap_y(packed, 1) + swap_y(packed, 3))
    inv_rms = lax.rsqrt(sums[rows + 16, rows : 2 * rows] / full + 1e-05)
    projected = inv_rms[:, None] * sums[:rows] - sums[rows : rows + 1]
    erased = (inv_rms[:, None] * gained - dot32_nt(projected, eraser_out)).astype(bf)
    sent = jnp.dot(placing, erased, preferred_element_type=f32).astype(bf)
    own = lax.all_to_all(sent.reshape(-1, capacity, width), "dp", split_axis=0, concat_axis=0, tiled=True)
    own = own.reshape(total, width)

    own, sums, inv_rms = lax.optimization_barrier((own, sums, inv_rms))

    mean_in = sums[rows : rows + 1]
    out_router_t = sums[rows + 8 : rows + 16]
    projected = inv_rms[:, None] * sums[:rows] - mean_in
    logits = inv_rms[:, None] * sums[rows + 16 : rows + 24, :rows].T - lax.dot_general(
        projected, out_router_t, (((1,), (1,)), ((), ())), precision=HIGHEST, preferred_element_type=f32
    )
    chosen = (expert_ids[:, :, None] == jnp.arange(E, dtype=jnp.int32)[None, None, :]).astype(f32)
    picked = jnp.sum(chosen * logits[:, None, :], axis=2)
    first_gate = jax.nn.sigmoid(picked[:, 0] - picked[:, 1])
    gate_pair = jnp.stack([first_gate, 1.0 - first_gate], axis=1)
    weights = jnp.sum((target[:, :, None] == place[None, None, :]).astype(f32) * gate_pair[:, :, None], axis=1)

    half = total // 2
    wg, wu, wd = w_gate[0], w_up[0], w_down[0]

    def rows_of(w, k, d):
        return lax.dynamic_slice(w, (first[2 * k + d], zero), (width, w.shape[1]))

    def cols_of(w, k, d):
        return lax.dynamic_slice(w, (zero, first[2 * k + d]), (w.shape[0], width))

    def dot(p, q):
        return jnp.dot(p, q, preferred_element_type=f32)

    def add_to(acc, *pieces):
        for piece, k, core in pieces:
            g = dot(piece, rows_of(wg, k, core))
            u = dot(piece, rows_of(wu, k, core))
            acc = (g, u) if acc is None else (acc[0] + g, acc[1] + u)
        return acc

    near1_b = swap_y(own[half:], 1)
    near3_a = swap_y(own[:half], 3)
    near1_a = swap_y(own[:half], 1)
    near3_b = swap_y(own[half:], 3)
    own2 = to_twin(own)
    acc = add_to(None, (own, 0, 0))
    acc = add_to(acc, (own2, 0, 1))
    far_a = swap_y(near3_a, 1)
    far_b = swap_y(near1_b, 3)
    near1 = jnp.concatenate([near1_a, near1_b], axis=0)
    near3 = jnp.concatenate([near3_a, near3_b], axis=0)
    near1, near3, acc = lax.optimization_barrier((near1, near3, acc))
    twin1 = to_twin(near1)
    twin3 = to_twin(near3)
    acc = add_to(acc, (near1, 1, 0), (near3, 3, 0), (twin1, 1, 1), (twin3, 3, 1))
    far_a, far_b, acc = lax.optimization_barrier((far_a, far_b, acc))
    far = jnp.concatenate([far_a, far_b], axis=0)
    far2 = to_twin(far)
    gate_act, up_act = add_to(acc, (far, 2, 0), (far2, 2, 1))
    hidden = (jax.nn.silu(gate_act) * up_act).astype(bf)

    def summed(k):
        other = dot(hidden, cols_of(wd, k, 1)).astype(bf)
        return dot(hidden, cols_of(wd, k, 0)) + to_twin(other).astype(f32)

    far = summed(2).astype(bf)
    got_a = swap_y(far[:half], 3)
    got_b = swap_y(far[half:], 1)
    to1 = summed(1)
    to3 = summed(3)
    from1_b = swap_y(to1[half:].astype(bf), 1)
    from3_a = swap_y(to3[:half].astype(bf), 3)
    mine = summed(0)
    from1_a = swap_y((to1[:half] + got_a.astype(f32)).astype(bf), 1)
    from3_b = swap_y((to3[half:] + got_b.astype(f32)).astype(bf), 3)
    reduced = mine + jnp.concatenate(
        [from1_a.astype(f32) + from3_a.astype(f32), from1_b.astype(f32) + from3_b.astype(f32)], axis=0
    )
    reduced, weights = lax.optimization_barrier((reduced.astype(bf), weights))
    returned = lax.all_to_all(
        reduced.reshape(-1, capacity, width), "dp", split_axis=0, concat_axis=0, tiled=True
    )
    mixed = jnp.dot(weights, returned.reshape(total, width).astype(f32), precision=HIGHEST, preferred_element_type=f32)
    return mixed.astype(bf)


def solution(mesh):
    in_specs = (
        P("dp", "tensor"),
        P("tensor"),
        P("tensor"),
        P("tensor", None),
        P("tensor", None),
        P("tensor", None),
        P("dp", None),
        P("dp", None),
        P("dp", None, "tensor"),
        P("dp", None, "tensor"),
        P("dp", "tensor", None),
    )

    return jax.shard_map(on_device, mesh=mesh, in_specs=in_specs, out_specs=P("dp", "tensor"), check_vma=False)
```

```python
import jax
import jax.numpy as jnp
from jax import lax
from jax.experimental import pallas as pl
from jax.experimental.pallas import tpu as pltpu
from jax.sharding import PartitionSpec as P

E = 8
HIGHEST = lax.Precision.HIGHEST


def dot32(a, b):
    return jnp.dot(a, b, precision=HIGHEST, preferred_element_type=jnp.float32)


def dot32_nt(a, b):
    return lax.dot_general(a, b, (((1,), (1,)), ((), ())), precision=HIGHEST, preferred_element_type=jnp.float32)


def sums_kernel(tokens, gain, mean, eraser_in, eraser_out, router_t, out, gained_out, eraser_out_copy):
    rows = tokens.shape[0]
    values = tokens[...].astype(jnp.float32)
    gained = values * gain[...]
    out[:rows] = dot32(gained, eraser_in[...])
    out[rows : rows + 8] = dot32(jnp.broadcast_to(mean[...], (8, mean.shape[1])), eraser_in[...])
    out[rows + 8 : rows + 16] = dot32(router_t[...], eraser_out[...])
    gained_out[...] = gained
    eraser_out_copy[...] = eraser_out[...]
    out[rows + 16 : rows + 24, :rows] = dot32_nt(router_t[...], gained)
    out[rows + 16 : rows + 24, rows : 2 * rows] = dot32_nt(jnp.ones((8, values.shape[1]), jnp.float32), values * values)


def load_kernel(near_first, far_first, gate, up, down, gate_rows, up_rows, down_cols, sems):
    near = pl.multiple_of(near_first[0], gate_rows.shape[0])
    far = pl.multiple_of(far_first[0], down_cols.shape[1])
    copies = (
        pltpu.make_async_copy(gate.at[0, pl.ds(near, gate_rows.shape[0])], gate_rows, sems.at[0]),
        pltpu.make_async_copy(up.at[0, pl.ds(near, up_rows.shape[0])], up_rows, sems.at[1]),
        pltpu.make_async_copy(down.at[0, :, pl.ds(far, down_cols.shape[1])], down_cols, sems.at[2]),
    )
    for copy in copies:
        copy.start()
    for copy in copies:
        copy.wait()


def on_device(tokens, norm_gain, eraser_mean, eraser_in, eraser_out, router, expert_ids, slots, w_gate, w_up, w_down):
    bf = jnp.bfloat16
    f32 = jnp.float32
    n_t = lax.axis_size("tensor")
    part_count = lax.axis_size("dp") // E
    rows, width = tokens.shape
    capacity = 3 * rows // 8
    full = width * n_t
    total = lax.axis_size("dp") * capacity
    rank = eraser_in.shape[1]
    t = lax.axis_index("tensor").astype(jnp.uint32)
    first = [(t ^ jnp.uint32(v)) * jnp.uint32(width) for v in range(n_t)]
    zero = t & jnp.uint32(0)
    core_rows = (t & jnp.uint32(1)) * jnp.uint32(width)
    twin_rows = jnp.uint32(width) - core_rows
    chip = (t >> jnp.uint32(1)).astype(jnp.int32)
    pair_first = (chip * (2 * width)).reshape(1)
    far_first = ((chip ^ 2) * (2 * width)).reshape(1)
    tokens, zero, core_rows, twin_rows, pair_first, far_first, *first = lax.optimization_barrier(
        (tokens, zero, core_rows, twin_rows, pair_first, far_first, *first)
    )

    def swap_y(v, k):
        return lax.ppermute(v, "tensor", [(s, s ^ (2 * k)) for s in range(n_t)])

    def to_twin(v):
        return lax.ppermute(v, "tensor", [(s, s ^ 1) for s in range(n_t)])

    target = jnp.where(slots < capacity, expert_ids * capacity + slots, -1)
    place = jnp.arange(total, dtype=jnp.int32)
    place = (place // capacity // part_count) * capacity + place % capacity
    match = target.T[:, None, :] == place[None, :, None]
    placing = lax.optimization_barrier(jnp.any(match, axis=0).astype(bf))
    packed, gained, eraser_out = pl.pallas_call(
        sums_kernel,
        out_shape=[pltpu.VMEM((rows + 24, rank), f32), pltpu.VMEM((rows, width), f32), pltpu.VMEM((width, rank), f32)],
        out_specs=[pl.BlockSpec(memory_space=pltpu.VMEM)] * 3,
        name="sums",
    )(tokens, norm_gain[None, :], eraser_mean[None, :], eraser_in, eraser_out, router.T)
    pair_shapes = [(2 * width, w_gate.shape[2])] * 2 + [(w_down.shape[1], 2 * width)]
    pair_gate, pair_up, far_down = pl.pallas_call(
        load_kernel,
        in_specs=[
            pl.BlockSpec(memory_space=pltpu.SMEM),
            pl.BlockSpec(memory_space=pltpu.SMEM),
            pl.BlockSpec(memory_space=pltpu.HBM),
            pl.BlockSpec(memory_space=pltpu.HBM),
            pl.BlockSpec(memory_space=pltpu.HBM),
        ],
        out_shape=[pltpu.VMEM(shape, bf) for shape in pair_shapes],
        out_specs=[pl.BlockSpec(memory_space=pltpu.VMEM)] * 3,
        scratch_shapes=[pltpu.SemaphoreType.DMA((3,))],
        compiler_params=pltpu.CompilerParams(vmem_limit_bytes=56 << 20),
        name="load",
    )(pair_first, far_first, w_gate, w_up, w_down)
    packed = packed + to_twin(packed)
    sums = (packed + swap_y(packed, 2)) + (swap_y(packed, 1) + swap_y(packed, 3))
    inv_rms = lax.rsqrt(sums[rows + 16, rows : 2 * rows] / full + 1e-05)
    projected = inv_rms[:, None] * sums[:rows] - sums[rows : rows + 1]
    erased = (inv_rms[:, None] * gained - dot32_nt(projected, eraser_out)).astype(bf)
    sent = jnp.dot(placing, erased, preferred_element_type=f32).astype(bf)
    own = lax.all_to_all(sent.reshape(-1, capacity, width), "dp", split_axis=0, concat_axis=0, tiled=True)
    own = own.reshape(total, width)

    own, sums, inv_rms = lax.optimization_barrier((own, sums, inv_rms))

    mean_in = sums[rows : rows + 1]
    out_router_t = sums[rows + 8 : rows + 16]
    projected = inv_rms[:, None] * sums[:rows] - mean_in
    logits = inv_rms[:, None] * sums[rows + 16 : rows + 24, :rows].T - lax.dot_general(
        projected, out_router_t, (((1,), (1,)), ((), ())), precision=HIGHEST, preferred_element_type=f32
    )
    chosen = (expert_ids[:, :, None] == jnp.arange(E, dtype=jnp.int32)[None, None, :]).astype(f32)
    picked = jnp.sum(chosen * logits[:, None, :], axis=2)
    first_gate = jax.nn.sigmoid(picked[:, 0] - picked[:, 1])
    gate_pair = jnp.stack([first_gate, 1.0 - first_gate], axis=1)
    weights = jnp.sum((target[:, :, None] == place[None, None, :]).astype(f32) * gate_pair[:, :, None], axis=1)

    half = total // 2
    wg, wu, wd = w_gate[0], w_up[0], w_down[0]

    def rows_of(w, k, d):
        return lax.dynamic_slice(w, (first[2 * k + d], zero), (width, w.shape[1]))

    def cols_of(w, k, d):
        return lax.dynamic_slice(w, (zero, first[2 * k + d]), (w.shape[0], width))

    def far_cols(begin):
        return lax.dynamic_slice(far_down, (zero, begin), (far_down.shape[0], width))

    def dot(p, q):
        return jnp.dot(p, q, preferred_element_type=f32)

    def add_to(acc, *pieces):
        for piece, k, core in pieces:
            g = dot(piece, rows_of(wg, k, core))
            u = dot(piece, rows_of(wu, k, core))
            acc = (g, u) if acc is None else (acc[0] + g, acc[1] + u)
        return acc

    near1_b = swap_y(own[half:], 1)
    near3_a = swap_y(own[:half], 3)
    near1_a = swap_y(own[:half], 1)
    near3_b = swap_y(own[half:], 3)
    own2 = to_twin(own)
    acc = tuple(dot(own, lax.dynamic_slice(w, (core_rows, zero), (width, w.shape[1]))) for w in (pair_gate, pair_up))
    acc = tuple(
        part + dot(own2, lax.dynamic_slice(w, (twin_rows, zero), (width, w.shape[1])))
        for part, w in zip(acc, (pair_gate, pair_up))
    )
    far_a = swap_y(near3_a, 1)
    far_b = swap_y(near1_b, 3)
    near1 = jnp.concatenate([near1_a, near1_b], axis=0)
    near3 = jnp.concatenate([near3_a, near3_b], axis=0)
    near1, near3, acc = lax.optimization_barrier((near1, near3, acc))
    twin1 = to_twin(near1)
    twin3 = to_twin(near3)
    acc = add_to(acc, (near1, 1, 0), (near3, 3, 0), (twin1, 1, 1), (twin3, 3, 1))
    far_a, far_b, acc = lax.optimization_barrier((far_a, far_b, acc))
    far = jnp.concatenate([far_a, far_b], axis=0)
    far2 = to_twin(far)
    gate_act, up_act = add_to(acc, (far, 2, 0), (far2, 2, 1))
    hidden = (jax.nn.silu(gate_act) * up_act).astype(bf)

    def summed(k):
        other = dot(hidden, far_cols(twin_rows) if k == 2 else cols_of(wd, k, 1)).astype(bf)
        return dot(hidden, far_cols(core_rows) if k == 2 else cols_of(wd, k, 0)) + to_twin(other).astype(f32)

    far = summed(2).astype(bf)
    got_a = swap_y(far[:half], 3)
    got_b = swap_y(far[half:], 1)
    to1 = summed(1)
    to3 = summed(3)
    from1_b = swap_y(to1[half:].astype(bf), 1)
    from3_a = swap_y(to3[:half].astype(bf), 3)
    mine = summed(0)
    from1_a = swap_y((to1[:half] + got_a.astype(f32)).astype(bf), 1)
    from3_b = swap_y((to3[half:] + got_b.astype(f32)).astype(bf), 3)
    reduced = mine + jnp.concatenate(
        [from1_a.astype(f32) + from3_a.astype(f32), from1_b.astype(f32) + from3_b.astype(f32)], axis=0
    )
    high = lax.reduce_precision(weights, 8, 7)
    terms = jnp.concatenate([high, weights - high], axis=0).astype(bf)
    reduced, terms = lax.optimization_barrier((reduced.astype(bf), terms))
    returned = lax.all_to_all(
        reduced.reshape(-1, capacity, width), "dp", split_axis=0, concat_axis=0, tiled=True
    ).reshape(total, width)
    mixed = jnp.dot(terms, returned, preferred_element_type=f32)
    return (mixed[:rows] + mixed[rows:]).astype(bf)


def solution(mesh):
    in_specs = (
        P("dp", "tensor"),
        P("tensor"),
        P("tensor"),
        P("tensor", None),
        P("tensor", None),
        P("tensor", None),
        P("dp", None),
        P("dp", None),
        P("dp", None, "tensor"),
        P("dp", None, "tensor"),
        P("dp", "tensor", None),
    )

    return jax.shard_map(on_device, mesh=mesh, in_specs=in_specs, out_specs=P("dp", "tensor"), check_vma=False)
```
